32 devices in a mesh: prob: 1 (over z), feat: 32 (over y, x, core).
Axes of the slice: x: 4, y: 4, z: 1, core: 2. Of those that a mesh axis runs over, the one named last changes fastest.
The devices are a block of a 4x4x8 slice.
Arguments:
- design: bfloat16 [16384, 32768], P('prob', 'feat')
- targets: float32 [16384, 100], P('prob')
- weights_init: float32 [32768, 100], P(('prob', 'feat'))
- step_sizes: float32 [32768], P(('prob', 'feat'))
Outputs:
- output 1: float32 [32768, 100], P(('prob', 'feat'))
- output 2: float32 [16384, 100], P('prob')
All inputs are finite; a program needn't handle non-finite values.
Results may differ from the reference program's by a relative error of at most 0.001.
Values are sent between devices in bfloat16 or wider.
A program may use at most 768 MiB of HBM per device.

```python
import jax
import jax.numpy as jnp
from jax import lax

SAMPLES = 16384
TARGETS = 100
FEATURES = 32768
SWEEPS = 6
SPIKE_RANK = 4
RIDGE_COEF = 1.0
MIX_WEIGHT = 0.75
STEP_TOTAL = 2.0


def spectral_bound(design, step_gain, rng_key):
    ridge_val = RIDGE_COEF / SAMPLES

    def apply_op(probe_vec):
        proj_rows = jnp.dot(design, probe_vec.astype(jnp.bfloat16), preferred_element_type=jnp.float32)
        back_cols = jnp.dot(proj_rows.astype(jnp.bfloat16), design, preferred_element_type=jnp.float32)
        return step_gain * (back_cols / SAMPLES + ridge_val * probe_vec)

    def power_step(step_idx, probe_vec):
        image_vec = apply_op(probe_vec)
        return image_vec / jnp.linalg.norm(image_vec)

    start_vec = jax.random.normal(rng_key, (FEATURES,), jnp.float32)
    probe_vec = lax.fori_loop(0, 24, power_step, start_vec / jnp.linalg.norm(start_vec))
    return jnp.linalg.norm(apply_op(probe_vec))


def setup_inputs(seed: int = 0, part: int = 0) -> dict:
    sub_keys = jax.random.split(jax.random.fold_in(jax.random.key(seed), part), 8)
    bulk_edge = (SAMPLES ** -0.5 + FEATURES ** -0.5) ** 2
    spike_amp = (2.0 * bulk_edge) ** 0.5
    noise_mat = jax.random.normal(sub_keys[0], (SAMPLES, FEATURES), jnp.float32)
    factors = jax.random.normal(sub_keys[1], (SAMPLES, SPIKE_RANK), jnp.float32)
    loadings = jax.random.normal(sub_keys[2], (SPIKE_RANK, FEATURES), jnp.float32)
    dense_x = (noise_mat + spike_amp * jnp.dot(factors, loadings)) * FEATURES ** -0.5
    design = dense_x.astype(jnp.bfloat16)
    coef_true = jax.random.normal(sub_keys[3], (FEATURES, TARGETS), jnp.float32)
    targets = jnp.dot(dense_x, coef_true) + 0.5 * jax.random.normal(sub_keys[4], (SAMPLES, TARGETS), jnp.float32)
    weights_init = jax.random.normal(sub_keys[5], (FEATURES, TARGETS), jnp.float32)
    step_gain = jax.random.uniform(sub_keys[6], (FEATURES,), jnp.float32, 0.25, 1.75)
    top_eig = spectral_bound(design, step_gain, sub_keys[7])
    step_sizes = step_gain * (STEP_TOTAL / SWEEPS) / (1.15 * top_eig)
    return {'design': design, 'targets': targets, 'weights_init': weights_init, 'step_sizes': step_sizes}


def reference(design, targets, weights_init, step_sizes):
    ridge_val = RIDGE_COEF / SAMPLES
    step_col = step_sizes[:, None]
    residual = targets - jnp.dot(design, weights_init.astype(jnp.bfloat16), preferred_element_type=jnp.float32)

    def one_sweep(state_pair, unused):
        weights, residual = state_pair
        gradient = lax.dot_general(design, residual.astype(jnp.bfloat16), (((0,), (0,)), ((), ())), preferred_element_type=jnp.float32) / SAMPLES
        update = step_col * (gradient - ridge_val * weights)
        weights = weights + MIX_WEIGHT * update
        residual = residual - MIX_WEIGHT * jnp.dot(design, update.astype(jnp.bfloat16), preferred_element_type=jnp.float32)
        return (weights, residual), None

    (weights, residual), unused_out = lax.scan(one_sweep, (weights_init, residual), None, length=SWEEPS)
    return weights, residual
```

```python
import functools
import math

import jax
import jax.numpy as jnp
from jax import lax
from jax.experimental import pallas as pl
from jax.experimental.pallas import tpu as pltpu
from jax.sharding import PartitionSpec as P

SWEEPS = 6
RIDGE_COEF = 1.0
MIX_WEIGHT = 0.75
CHUNKS = 4
CORES = 2
MESH = pl.DeviceIdType.MESH


class _Copy:
    def __init__(self, *args):
        self.args = args

    def _make(self):
        src, dst, send_sem, recv_sem, device = self.args
        return pltpu.make_async_remote_copy(src_ref=src, dst_ref=dst, send_sem=send_sem, recv_sem=recv_sem,
                                            device_id=device, device_id_type=MESH)

    def start(self):
        self._make().start()

    def wait_recv(self):
        self._make().wait_recv()

    def wait_send(self):
        self._make().wait_send()


def _up(v, m):
    return (v + m - 1) // m * m


def _split(v, m):
    top = _up(v // 2, m)
    return top, v - top


def _kernel(n, side, kf, kb, x_hbm, y_ref, w0_ref, eta_ref, w_ref, r_hbm,
            xv, c_buf, d_buf, far1, near1, far2, near2, t_buf, rt, own, gacc, dwt,
            send, recv, load_sem, out_sem, free):
    q_all = CHUNKS
    rows = n // q_all
    half = rows // CORES
    w1 = half // side
    w2 = w1 // side
    ka, kc = _split(kf, 8)
    ba, bc = _split(kb, 16)
    last = SWEEPS

    me = lax.axis_index('feat')
    core = lax.rem(me, CORES)
    px = lax.rem(me // CORES, side)
    py = me // (CORES * side)
    peer = 1 - core
    hbase = pl.multiple_of(core * half, half)
    pbase = pl.multiple_of(peer * half, half)

    def dev(yy, xx, cc):
        return {'feat': (yy * side + xx) * CORES + cc}

    def step(v, s):
        return lax.rem(v + (s + side), side)

    xp, xm = dev(py, step(px, 1), core), dev(py, step(px, -1), core)
    yp, ym = dev(step(py, 1), px, core), dev(step(py, -1), px, core)
    mate = dev(py, px, peer)
    rings = [((px, xp, xm), (py, yp, ym)) if q % 2 == 0 else ((py, yp, ym), (px, xp, xm)) for q in range(q_all)]

    barrier = pltpu.get_barrier_semaphore()
    for d in (xp, xm, yp, ym, mate):
        pl.semaphore_signal(barrier, inc=1, device_id=d, device_id_type=MESH)

    def load(q, cc):
        def one(i, carry):
            a, b = i // side, lax.rem(i, side)
            d = ((b * side + a) if q % 2 == 0 else (a * side + b)) * CORES + cc
            src = x_hbm.at[pl.ds(pl.multiple_of(d * (q_all * w2) + q * w2, w2), w2), :]
            dst = xv.at[q, pl.ds(pl.multiple_of(cc * half + i * w2, w2), w2), :]
            pltpu.make_async_copy(src, dst, load_sem.at[q, cc]).start()
            return carry
        lax.fori_loop(0, side * side, one, 0)

    def load_wait(q, cc, base):
        ref = xv.at[q, pl.ds(base, half), :]
        pltpu.make_async_copy(ref, ref, load_sem.at[q, cc]).wait()

    for q in range(q_all):
        load(q, peer)
        load(q, core)

    own[...] = y_ref[...]
    w_ref[...] = w0_ref[...]
    dwt[...] = w0_ref[...].astype(jnp.bfloat16)
    pl.semaphore_wait(barrier, 5)

    def rc(src, dst, q, k, device):
        return _Copy(src, dst, send.at[q, k], recv.at[q, k], device)

    def lanes(base, width):
        return pl.ds(pl.multiple_of(base, 128), width)

    def c_d2d(q):
        return rc(c_buf.at[q, :, lanes(pbase, half)], d_buf.at[q], q, 0, mate)

    def rs_copies(q, stage):
        idx, plus, minus = rings[q][stage]
        if stage == 0:
            src, width, far, near = d_buf.at[q], w1, far1, near1
        else:
            src, width, far, near = t_buf.at[q], w2, far2, near2
        k0 = 1 + 6 * stage

        def cut(i, lo, size):
            return src.at[pl.ds(lo, size), lanes(i * width, width)]

        f, p, m = step(idx, 2), step(idx, 1), step(idx, -1)
        return dict(
            far=(rc(cut(f, 0, ka), far.at[q, 0], q, k0, plus),
                 rc(cut(f, ka, kc), far.at[q, 1, pl.ds(0, kc), :], q, k0 + 1, minus)),
            plain=(rc(cut(p, ka, kc), near.at[q, 0, pl.ds(ka, kc), :], q, k0 + 2, plus),
                   rc(cut(m, 0, ka), near.at[q, 1, pl.ds(0, ka), :], q, k0 + 3, minus)),
            aug=(rc(cut(p, 0, ka), near.at[q, 0, pl.ds(0, ka), :], q, k0 + 4, plus),
                 rc(cut(m, ka, kc), near.at[q, 1, pl.ds(ka, kc), :], q, k0 + 5, minus)))

    def start(copies):
        for c in copies:
            c.start()

    def recv_wait(copies):
        for c in copies:
            c.wait_recv()

    def send_wait(copies):
        for c in copies:
            c.wait_send()

    def rs_first(q, stage):
        cp = rs_copies(q, stage)
        start(cp['far'])
        start(cp['plain'])

    def rs_mid(q, stage):
        idx = rings[q][stage][0]
        src, width, far = (d_buf, w1, far1) if stage == 0 else (t_buf, w2, far2)
        cp = rs_copies(q, stage)
        p, m = step(idx, 1), step(idx, -1)
        cp['far'][0].wait_recv()
        at = (q, pl.ds(0, ka), lanes(p * width, width))
        src[at] = src[at] + far[q, 0]
        cp['aug'][0].start()
        cp['far'][1].wait_recv()
        at = (q, pl.ds(ka, kc), lanes(m * width, width))
        src[at] = src[at] + far[q, 1, pl.ds(0, kc), :]
        cp['aug'][1].start()

    def rs_total(q, stage):
        idx = rings[q][stage][0]
        src, width, near = (d_buf, w1, near1) if stage == 0 else (t_buf, w2, near2)
        cp = rs_copies(q, stage)
        recv_wait(cp['plain'])
        recv_wait(cp['aug'])
        return src[q, :, lanes(idx * width, width)] + (near[q, 0] + near[q, 1])

    def ag_copies(q, wide):
        (i1, p1, m1), (i2, p2, m2) = rings[q]
        buf, top, low = (c_buf, ka, kc) if wide else (rt, ba, bc)
        b0 = hbase + i1 * w1

        def cut(base, width, part):
            r = {None: slice(None), 0: pl.ds(0, top), 1: pl.ds(top, low)}[part]
            return buf.at[q, r, lanes(base, width)]

        def to(base, width, part, k, device):
            ref = cut(base, width, part)
            return rc(ref, ref, q, k, device)

        a, b = step(i2, -1), step(i2, 1)
        c, d, e = step(i1, -1), step(i1, 1), step(i1, 2)
        out = dict(
            n1=(to(b0 + i2 * w2, w2, None, 13, p2), to(b0 + i2 * w2, w2, None, 14, m2)),
            f1=(to(b0 + a * w2, w2, 0, 15, p2), to(b0 + b * w2, w2, 1, 16, m2)),
            n2=(to(b0, w1, None, 17, p1), to(b0, w1, None, 18, m1)),
            f2=(to(hbase + c * w1, w1, 0, 19, p1), to(hbase + d * w1, w1, 1, 20, m1)))
        out['x'] = tuple(to(hbase + i * w1, w1, None, 21 + j, mate) for j, i in enumerate((i1, c, d, e)))
        return out

    def ag_first(q, wide):
        start(ag_copies(q, wide)['n1'])

    def ag_fwd1(q, wide):
        cp = ag_copies(q, wide)
        for a, b in zip(cp['n1'], cp['f1']):
            a.wait_recv()
            b.start()

    def ag_second(q, wide):
        cp = ag_copies(q, wide)
        recv_wait(cp['f1'])
        start(cp['n2'])
        if wide:
            pl.semaphore_wait(free.at[q], 1)
        cp['x'][0].start()

    def ag_fwd2(q, wide):
        cp = ag_copies(q, wide)
        for a, b in zip(cp['n2'], cp['f2']):
            a.wait_recv()
            b.start()
        start(cp['x'][1:3])

    def ag_last(q, wide):
        cp = ag_copies(q, wide)
        recv_wait(cp['f2'])
        cp['x'][3].start()

    def ag_mate(q, wide):
        recv_wait(ag_copies(q, wide)['x'])

    def partial_product(q, base):
        v = lax.dot_general(dwt[...], xv[q, pl.ds(base, half), :], (((1,), (1,)), ((), ())),
                            preferred_element_type=jnp.float32)
        c_buf[q, :, pl.ds(base, half)] = v[:kf]

    def gradient(q, base):
        gacc[...] += jnp.dot(rt[q, :, pl.ds(base, half)], xv[q, pl.ds(base, half), :],
                             preferred_element_type=jnp.float32)

    def sweep(t, carry):
        first = t == 0
        scale = jnp.where(first, jnp.float32(1.0), jnp.float32(MIX_WEIGHT))

        def gathers(f, q):
            @pl.when(t < last)
            def _():
                f(q, False)

            @pl.when(t == last)
            def _():
                f(q, True)

        def product(q, mates):
            @pl.when(first)
            def _():
                load_wait(q, peer if mates else core, pbase if mates else hbase)
            partial_product(q, pbase if mates else hbase)
            if mates:
                c_d2d(q).start()

        def pair_sum(q):
            c_d2d(q).wait_recv()
            d_buf[q] = d_buf[q] + c_buf[q, :, pl.ds(hbase, half)]
            rs_first(q, 0)

        def sent(q, stage):
            cp = rs_copies(q, stage)
            for key in ('far', 'plain', 'aug'):
                send_wait(cp[key])

        def ring_sum(q):
            t_buf[q] = rs_total(q, 0)
            rs_first(q, 1)
            c_d2d(q).wait_send()

            @pl.when(t == last)
            def _():
                pl.semaphore_signal(free.at[q], inc=1, device_id=mate, device_id_type=MESH)

        def finish(q):
            fresh = own[q, pl.ds(0, kf), :] - scale * rs_total(q, 1)
            own[q, pl.ds(0, kf), :] = fresh
            sent(q, 0)
            idx = rings[q]
            at = lanes(hbase + idx[0][0] * w1 + idx[1][0] * w2, w2)

            @pl.when(t < last)
            def _():
                rt[q, :, at] = own[q].astype(jnp.bfloat16)

            @pl.when(t == last)
            def _():
                c_buf[q, :, at] = own[q, pl.ds(0, kf), :]
            gathers(ag_first, q)

        product(0, True)
        product(0, False)
        product(1, True)
        pair_sum(0)
        product(1, False)
        pair_sum(1)
        product(2, True)
        product(2, False)
        rs_mid(0, 0)
        product(3, True)
        rs_mid(1, 0)
        product(3, False)
        pair_sum(2)
        pair_sum(3)
        ring_sum(0)
        ring_sum(1)
        rs_mid(0, 1)
        rs_mid(1, 1)
        rs_mid(2, 0)
        rs_mid(3, 0)
        finish(0)
        finish(1)
        gathers(ag_fwd1, 0)
        gathers(ag_fwd1, 1)
        ring_sum(2)
        ring_sum(3)
        gathers(ag_second, 0)
        gathers(ag_second, 1)
        rs_mid(2, 1)
        rs_mid(3, 1)
        gathers(ag_fwd2, 0)
        gathers(ag_fwd2, 1)
        finish(2)
        finish(3)
        gathers(ag_fwd1, 2)
        gathers(ag_fwd1, 3)
        gathers(ag_last, 0)
        gathers(ag_last, 1)
        gathers(ag_second, 2)
        gathers(ag_second, 3)

        @pl.when(t < last)
        def _():
            gacc[...] = jnp.zeros_like(gacc)
            gradient(0, hbase)
            gradient(1, hbase)
        gathers(ag_mate, 0)
        gathers(ag_mate, 1)
        gathers(ag_fwd2, 2)
        gathers(ag_fwd2, 3)

        @pl.when(t < last)
        def _():
            gradient(0, pbase)
            gradient(1, pbase)
        gathers(ag_last, 2)
        gathers(ag_last, 3)

        @pl.when(t < last)
        def _():
            gradient(2, hbase)
            gradient(3, hbase)
        gathers(ag_mate, 2)
        gathers(ag_mate, 3)

        def drain(q, wide):
            cp = ag_copies(q, wide)
            for key in ('n1', 'f1', 'n2', 'f2', 'x'):
                send_wait(cp[key])

        for q in range(q_all):
            sent(q, 1)
            gathers(drain, q)

        @pl.when(t < last)
        def _():
            gradient(2, pbase)
            gradient(3, pbase)
            update = eta_ref[...] * (gacc[...] * (1.0 / n) - (RIDGE_COEF / n) * w_ref[...])
            w_ref[...] = w_ref[...] + MIX_WEIGHT * update
            dwt[...] = update.astype(jnp.bfloat16)
        return carry

    lax.fori_loop(0, last + 1, sweep, 0)

    def piece(i, carry):
        for q in range(q_all):
            cc, j = i // (side * side), lax.rem(i, side * side)
            a, b = j // side, lax.rem(j, side)
            d = ((b * side + a) if q % 2 == 0 else (a * side + b)) * CORES + cc
            pltpu.make_async_copy(c_buf.at[q, :, lanes(i * w2, w2)],
                                  r_hbm.at[:, lanes((d * q_all + q) * w2, w2)], out_sem).start()
        return carry
    lax.fori_loop(0, CORES * side * side, piece, 0)
    for q in range(q_all):
        pltpu.make_async_copy(c_buf.at[q], c_buf.at[q], out_sem).wait()


def solution(mesh):
    group = mesh.shape['feat']
    side = math.isqrt(group // CORES)

    def local_solve(design, targets, weights, step_sizes):
        n, feats = design.shape
        k = targets.shape[1]
        kf, kb = _up(k, 8), _up(k, 16)
        rows = n // CHUNKS
        half = rows // CORES
        w1 = half // side
        w2 = w1 // side
        ka = _split(kf, 8)[0]
        share = n // group
        me = lax.axis_index('feat')
        mine = lax.dynamic_slice_in_dim(targets, me * share, share, 0)
        mine = jnp.pad(jnp.swapaxes(mine.reshape(CHUNKS, w2, k), 1, 2), ((0, 0), (0, kb - k), (0, 0)))
        wt = jnp.pad(weights.T, ((0, kb - k), (0, 0)))
        f32, bf16 = jnp.float32, jnp.bfloat16
        vm = pl.BlockSpec(memory_space=pltpu.VMEM)
        hb = pl.BlockSpec(memory_space=pl.ANY)
        w_out, r_out = pl.pallas_call(
            functools.partial(_kernel, n, side, kf, kb),
            out_shape=(jax.ShapeDtypeStruct((kb, feats), f32), jax.ShapeDtypeStruct((kf, n), f32)),
            in_specs=[hb, vm, vm, vm],
            out_specs=(vm, hb),
            scratch_shapes=[
                pltpu.VMEM((CHUNKS, rows, feats), bf16),
                pltpu.VMEM((CHUNKS, kf, rows), f32),
                pltpu.VMEM((CHUNKS, kf, half), f32),
                pltpu.VMEM((CHUNKS, 2, ka, w1), f32),
                pltpu.VMEM((CHUNKS, 2, kf, w1), f32),
                pltpu.VMEM((CHUNKS, 2, ka, w2), f32),
                pltpu.VMEM((CHUNKS, 2, kf, w2), f32),
                pltpu.VMEM((CHUNKS, kf, w1), f32),
                pltpu.VMEM((CHUNKS, kb, rows), bf16),
                pltpu.VMEM((CHUNKS, kb, w2), f32),
                pltpu.VMEM((kb, feats), f32),
                pltpu.VMEM((kb, feats), bf16),
                pltpu.SemaphoreType.DMA((CHUNKS, 25)),
                pltpu.SemaphoreType.DMA((CHUNKS, 25)),
                pltpu.SemaphoreType.DMA((CHUNKS, CORES)),
                pltpu.SemaphoreType.DMA,
                pltpu.SemaphoreType.REGULAR((CHUNKS,)),
            ],
            compiler_params=pltpu.CompilerParams(
                collective_id=0, has_side_effects=True, vmem_limit_bytes=67043328),
        )(design, mine, wt, step_sizes[None, :])
        return w_out[:k].T, r_out[:k].T

    return jax.shard_map(
        local_solve,
        mesh=mesh,
        in_specs=(P('prob', 'feat'), P('prob', None), P(('prob', 'feat'), None), P(('prob', 'feat'))),
        out_specs=(P(('prob', 'feat'), None), P('prob', None)),
        check_vma=False,
    )
```

```python
import functools
import math

import jax
import jax.numpy as jnp
from jax import lax
from jax.experimental import pallas as pl
from jax.experimental.pallas import tpu as pltpu
from jax.sharding import PartitionSpec as P

SWEEPS = 6
RIDGE_COEF = 1.0
MIX_WEIGHT = 0.75
CHUNKS = 4
CORES = 2
SCHEDULE = (
    'A0 B0 A1 B1', 'S0 S1 P0 O0', 'P1 N0 O1 N1', 'A2 B2 A3 B3', 'a0 a1 P2 O2', 'S2 S3 P3 O3', 'p0 o0 p1 o1',
    'N2 N3 s0 s1', 'T0 T1 p2 o2', 'p3 o3 s2 s3', 'a2 a3 b0 b1', 'T2 T3 F0 F1', 'b2 b3 c0 c1', 'F2 F3 d0 d1',
    'c2 c3 e0 e1', 'k0 k1 G0 G1', 'd2 d3 m0 m1', 'f0 f1 H0 H1', 'e2 e3 k2 k3', 'g0 g1 n0 n1', 'h0 h1 G2 G3',
    'f2 f3 m2 m3', 'H2 H3 g2 g3', 'D0 D1 D2 D3', 'n2 n3 h2 h3',
)
MESH = pl.DeviceIdType.MESH


class _Copy:
    def __init__(self, *args):
        self.args = args

    def _make(self):
        src, dst, send_sem, recv_sem, device = self.args
        return pltpu.make_async_remote_copy(src_ref=src, dst_ref=dst, send_sem=send_sem, recv_sem=recv_sem,
                                            device_id=device, device_id_type=MESH)

    def start(self):
        self._make().start()

    def wait_recv(self):
        self._make().wait_recv()

    def wait_send(self):
        self._make().wait_send()


def _up(v, m):
    return (v + m - 1) // m * m


def _split(v, m):
    top = _up(v // 2, m)
    return top, v - top


def _kernel(n, side, kf, kb, x_hbm, y_ref, w0_ref, eta_ref, w_ref, r_hbm,
            xv, c_buf, d_buf, far1, near1, far2, near2, t_buf, rt, own, gacc, dwt,
            send, recv, load_sem, out_sem, free):
    q_all = CHUNKS
    rows = n // q_all
    half = rows // CORES
    w1 = half // side
    w2 = w1 // side
    ka, kc = _split(kf, 8)
    ba, bc = _split(kb, 16)
    last = SWEEPS

    me = lax.axis_index('feat')
    core = lax.rem(me, CORES)
    px = lax.rem(me // CORES, side)
    py = me // (CORES * side)
    peer = 1 - core
    hbase = pl.multiple_of(core * half, half)
    pbase = pl.multiple_of(peer * half, half)

    def dev(yy, xx, cc):
        return {'feat': (yy * side + xx) * CORES + cc}

    def step(v, s):
        return lax.rem(v + (s + side), side)

    xp, xm = dev(py, step(px, 1), core), dev(py, step(px, -1), core)
    yp, ym = dev(step(py, 1), px, core), dev(step(py, -1), px, core)
    mate = dev(py, px, peer)
    rings = [((px, xp, xm), (py, yp, ym)) if q % 2 == 0 else ((py, yp, ym), (px, xp, xm)) for q in range(q_all)]

    barrier = pltpu.get_barrier_semaphore()
    for d in (xp, xm, yp, ym, mate):
        pl.semaphore_signal(barrier, inc=1, device_id=d, device_id_type=MESH)

    def load(q, cc):
        def one(i, carry):
            a, b = i // side, lax.rem(i, side)
            d = ((b * side + a) if q % 2 == 0 else (a * side + b)) * CORES + cc
            src = x_hbm.at[pl.ds(pl.multiple_of(d * (q_all * w2) + q * w2, w2), w2), :]
            dst = xv.at[q, pl.ds(pl.multiple_of(cc * half + i * w2, w2), w2), :]
            pltpu.make_async_copy(src, dst, load_sem.at[q, cc]).start()
            return carry
        lax.fori_loop(0, side * side, one, 0)

    def load_wait(q, cc, base):
        ref = xv.at[q, pl.ds(base, half), :]
        pltpu.make_async_copy(ref, ref, load_sem.at[q, cc]).wait()

    for q in range(q_all):
        load(q, peer)
        load(q, core)

    own[...] = y_ref[...]
    gacc[...] = jnp.zeros_like(gacc)
    w_ref[...] = w0_ref[...]
    dwt[...] = w0_ref[...].astype(jnp.bfloat16)
    pl.semaphore_wait(barrier, 5)

    def rc(src, dst, q, k, device):
        return _Copy(src, dst, send.at[q, k], recv.at[q, k], device)

    def lanes(base, width):
        return pl.ds(pl.multiple_of(base, 128), width)

    def blocks(q):
        idx = rings[q][0][0]
        return step(idx, 2), step(idx, 1), step(idx, -1), idx

    def c_d2d(q, j):
        at = blocks(q)[j] * w1
        return rc(c_buf.at[q, :, lanes(pbase + at, w1)], d_buf.at[q, :, lanes(at, w1)], q, j, mate)

    def rs_copies(q, stage):
        idx, plus, minus = rings[q][stage]
        if stage == 0:
            src, width, far, near = d_buf.at[q], w1, far1, near1
        else:
            src, width, far, near = t_buf.at[q], w2, far2, near2
        k0 = 4 + 6 * stage

        def cut(i, lo, size):
            return src.at[pl.ds(lo, size), lanes(i * width, width)]

        f, p, m = step(idx, 2), step(idx, 1), step(idx, -1)
        return dict(
            far=(rc(cut(f, 0, ka), far.at[q, 0], q, k0, plus),
                 rc(cut(f, ka, kc), far.at[q, 1, pl.ds(0, kc), :], q, k0 + 1, minus)),
            plain=(rc(cut(p, ka, kc), near.at[q, 0, pl.ds(ka, kc), :], q, k0 + 2, plus),
                   rc(cut(m, 0, ka), near.at[q, 1, pl.ds(0, ka), :], q, k0 + 3, minus)),
            aug=(rc(cut(p, 0, ka), near.at[q, 0, pl.ds(0, ka), :], q, k0 + 4, plus),
                 rc(cut(m, ka, kc), near.at[q, 1, pl.ds(ka, kc), :], q, k0 + 5, minus)))

    def start(copies):
        for c in copies:
            c.start()

    def recv_wait(copies):
        for c in copies:
            c.wait_recv()

    def send_wait(copies):
        for c in copies:
            c.wait_send()

    def rs_mid(q, stage):
        idx = rings[q][stage][0]
        src, width, far = (d_buf, w1, far1) if stage == 0 else (t_buf, w2, far2)
        cp = rs_copies(q, stage)
        p, m = step(idx, 1), step(idx, -1)
        cp['far'][0].wait_recv()
        at = (q, pl.ds(0, ka), lanes(p * width, width))
        src[at] = src[at] + far[q, 0]
        cp['aug'][0].start()
        cp['far'][1].wait_recv()
        at = (q, pl.ds(ka, kc), lanes(m * width, width))
        src[at] = src[at] + far[q, 1, pl.ds(0, kc), :]
        cp['aug'][1].start()

    def rs_total(q, stage):
        idx = rings[q][stage][0]
        src, width, near = (d_buf, w1, near1) if stage == 0 else (t_buf, w2, near2)
        cp = rs_copies(q, stage)
        recv_wait(cp['plain'])
        recv_wait(cp['aug'])
        return src[q, :, lanes(idx * width, width)] + (near[q, 0] + near[q, 1])

    def ag_copies(q, wide):
        (i1, p1, m1), (i2, p2, m2) = rings[q]
        buf, top, low = (c_buf, ka, kc) if wide else (rt, ba, bc)
        b0 = hbase + i1 * w1

        def cut(base, width, part):
            r = {None: slice(None), 0: pl.ds(0, top), 1: pl.ds(top, low)}[part]
            return buf.at[q, r, lanes(base, width)]

        def to(base, width, part, k, device):
            ref = cut(base, width, part)
            return rc(ref, ref, q, k, device)

        a, b = step(i2, -1), step(i2, 1)
        c, d, e = step(i1, -1), step(i1, 1), step(i1, 2)
        pieces = (i2, a, b, step(i2, 2))
        return dict(
            n1=(to(b0 + i2 * w2, w2, None, 16, p2), to(b0 + i2 * w2, w2, None, 17, m2)),
            f1=(to(b0 + a * w2, w2, 0, 18, p2), to(b0 + b * w2, w2, 1, 19, m2)),
            n2=[(to(b0 + i * w2, w2, None, 20 + 2 * j, p1), to(b0 + i * w2, w2, None, 21 + 2 * j, m1))
                for j, i in enumerate(pieces)],
            f2=[(to(hbase + c * w1 + i * w2, w2, 0, 28 + 2 * j, p1), to(hbase + d * w1 + i * w2, w2, 1, 29 + 2 * j, m1))
                for j, i in enumerate(pieces)],
            x=[to(hbase + i * w1, w1, None, 36 + j, mate) for j, i in enumerate((i1, c, d, e))])

    def ag_first(q, wide):
        cp = ag_copies(q, wide)
        start(cp['n1'])
        start(cp['n2'][0])

    def ag_fwd1(q, wide):
        cp = ag_copies(q, wide)
        for j in (0, 1):
            cp['n1'][j].wait_recv()
            cp['f1'][j].start()
            start(cp['n2'][1 + j])

    def ag_second(q, wide):
        cp = ag_copies(q, wide)
        recv_wait(cp['f1'])
        start(cp['n2'][3])
        if wide:
            pl.semaphore_wait(free.at[q], 1)
        cp['x'][0].start()

    def ag_fwd2(q, wide):
        cp = ag_copies(q, wide)
        for j in range(3):
            for a, b in zip(cp['n2'][j], cp['f2'][j]):
                a.wait_recv()
                b.start()

    def ag_fwd3(q, wide):
        cp = ag_copies(q, wide)
        for a, b in zip(cp['n2'][3], cp['f2'][3]):
            a.wait_recv()
            b.start()
        start(cp['x'][1:3])

    def ag_last(q, wide):
        cp = ag_copies(q, wide)
        for pair in cp['f2']:
            recv_wait(pair)
        cp['x'][3].start()

    def ag_mate(q, wide):
        recv_wait(ag_copies(q, wide)['x'][:3])

    def ag_mate2(q, wide):
        recv_wait(ag_copies(q, wide)['x'][3:])

    def partial_product(q, base, js):
        for j in js:
            at = pl.ds(pl.multiple_of(base + blocks(q)[j] * w1, w1), w1)
            v = lax.dot_general(dwt[...], xv[q, at, :], (((1,), (1,)), ((), ())), preferred_element_type=jnp.float32)
            c_buf[q, :, at] = v[:kf]

    def gradient(q, base, js):
        total = None
        for j in js:
            at = pl.ds(pl.multiple_of(base + blocks(q)[j] * w1, w1), w1)
            v = jnp.dot(rt[q, :, at], xv[q, at, :], preferred_element_type=jnp.float32)
            total = v if total is None else total + v
        gacc[...] += total

    def sweep(t, carry):
        first = t == 0
        scale = jnp.where(first, jnp.float32(1.0), jnp.float32(MIX_WEIGHT))

        def gathers(f, q):
            @pl.when(t < last)
            def _():
                f(q, False)

            @pl.when(t == last)
            def _():
                f(q, True)

        def product(q, mates, js, opens=False):
            if opens:
                @pl.when(first)
                def _():
                    load_wait(q, peer, pbase)
                    load_wait(q, core, hbase)
            partial_product(q, pbase if mates else hbase, js)
            if mates:
                start([c_d2d(q, j) for j in js])

        def pair_sum(q, js, then):
            for j in js:
                c_d2d(q, j).wait_recv()
                at = blocks(q)[j] * w1
                d_buf[q, :, lanes(at, w1)] = d_buf[q, :, lanes(at, w1)] + c_buf[q, :, lanes(hbase + at, w1)]
            if then:
                start(rs_copies(q, 0)[then])

        def sent(q, stage):
            cp = rs_copies(q, stage)
            for key in ('far', 'plain', 'aug'):
                send_wait(cp[key])

        def ring_sum(q):
            t_buf[q] = rs_total(q, 0)
            start(rs_copies(q, 1)['far'])
            start(rs_copies(q, 1)['plain'])
            send_wait([c_d2d(q, j) for j in range(4)])

            @pl.when(t == last)
            def _():
                pl.semaphore_signal(free.at[q], inc=1, device_id=mate, device_id_type=MESH)

        def finish(q):
            fresh = own[q, pl.ds(0, kf), :] - scale * rs_total(q, 1)
            own[q, pl.ds(0, kf), :] = fresh
            sent(q, 0)
            idx = rings[q]
            at = lanes(hbase + idx[0][0] * w1 + idx[1][0] * w2, w2)

            @pl.when(t < last)
            def _():
                rt[q, :, at] = own[q].astype(jnp.bfloat16)

            @pl.when(t == last)
            def _():
                c_buf[q, :, at] = own[q, pl.ds(0, kf), :]
            gathers(ag_first, q)

        def grad(q, base, js):
            @pl.when(t < last)
            def _():
                gradient(q, base, js)

        def drain(q, wide):
            cp = ag_copies(q, wide)
            for key in ('n1', 'f1', 'x'):
                send_wait(cp[key])
            for pair in cp['n2'] + cp['f2']:
                send_wait(pair)

        def drained(q):
            sent(q, 1)
            gathers(drain, q)

        acts = {
            'A': lambda q: product(q, True, (0,), True), 'B': lambda q: product(q, False, (0,)),
            'P': lambda q: product(q, True, (1, 2)), 'O': lambda q: product(q, False, (1, 2)),
            'p': lambda q: product(q, True, (3,)), 'o': lambda q: product(q, False, (3,)),
            'S': lambda q: pair_sum(q, (0,), 'far'), 'N': lambda q: pair_sum(q, (1, 2), 'plain'),
            's': lambda q: pair_sum(q, (3,), None),
            'a': lambda q: rs_mid(q, 0), 'T': ring_sum, 'b': lambda q: rs_mid(q, 1), 'F': finish,
            'c': lambda q: gathers(ag_fwd1, q), 'd': lambda q: gathers(ag_second, q),
            'e': lambda q: gathers(ag_fwd2, q), 'k': lambda q: gathers(ag_fwd3, q), 'f': lambda q: gathers(ag_last, q),
            'm': lambda q: gathers(ag_mate, q), 'n': lambda q: gathers(ag_mate2, q),
            'G': lambda q: grad(q, hbase, (1, 2, 3)), 'g': lambda q: grad(q, hbase, (0,)),
            'H': lambda q: grad(q, pbase, (1, 2, 3)), 'h': lambda q: grad(q, pbase, (0,)),
            'D': drained,
        }
        for act in ' '.join(SCHEDULE).split():
            with jax.named_scope(act):
                acts[act[0]](int(act[1:]))

        @pl.when(t < last)
        def _():
            update = eta_ref[...] * (gacc[...] * (1.0 / n) - (RIDGE_COEF / n) * w_ref[...])
            w_ref[...] = w_ref[...] + MIX_WEIGHT * update
            dwt[...] = update.astype(jnp.bfloat16)
            gacc[...] = jnp.zeros_like(gacc)
        return carry

    lax.fori_loop(0, last + 1, sweep, 0)

    def piece(i, carry):
        for q in range(q_all):
            cc, j = i // (side * side), lax.rem(i, side * side)
            a, b = j // side, lax.rem(j, side)
            d = ((b * side + a) if q % 2 == 0 else (a * side + b)) * CORES + cc
            pltpu.make_async_copy(c_buf.at[q, :, lanes(i * w2, w2)],
                                  r_hbm.at[:, lanes((d * q_all + q) * w2, w2)], out_sem).start()
        return carry
    lax.fori_loop(0, CORES * side * side, piece, 0)
    for q in range(q_all):
        pltpu.make_async_copy(c_buf.at[q], c_buf.at[q], out_sem).wait()


def solution(mesh):
    group = mesh.shape['feat']
    side = math.isqrt(group // CORES)

    def local_solve(design, targets, weights, step_sizes):
        n, feats = design.shape
        k = targets.shape[1]
        kf, kb = _up(k, 8), _up(k, 16)
        rows = n // CHUNKS
        half = rows // CORES
        w1 = half // side
        w2 = w1 // side
        ka = _split(kf, 8)[0]
        share = n // group
        me = lax.axis_index('feat')
        mine = lax.dynamic_slice_in_dim(targets, me * share, share, 0)
        mine = jnp.pad(jnp.swapaxes(mine.reshape(CHUNKS, w2, k), 1, 2), ((0, 0), (0, kb - k), (0, 0)))
        wt = jnp.pad(weights.T, ((0, kb - k), (0, 0)))
        f32, bf16 = jnp.float32, jnp.bfloat16
        vm = pl.BlockSpec(memory_space=pltpu.VMEM)
        hb = pl.BlockSpec(memory_space=pl.ANY)
        w_out, r_out = pl.pallas_call(
            functools.partial(_kernel, n, side, kf, kb),
            out_shape=(jax.ShapeDtypeStruct((kb, feats), f32), jax.ShapeDtypeStruct((kf, n), f32)),
            in_specs=[hb, vm, vm, vm],
            out_specs=(vm, hb),
            scratch_shapes=[
                pltpu.VMEM((CHUNKS, rows, feats), bf16),
                pltpu.VMEM((CHUNKS, kf, rows), f32),
                pltpu.VMEM((CHUNKS, kf, half), f32),
                pltpu.VMEM((CHUNKS, 2, ka, w1), f32),
                pltpu.VMEM((CHUNKS, 2, kf, w1), f32),
                pltpu.VMEM((CHUNKS, 2, ka, w2), f32),
                pltpu.VMEM((CHUNKS, 2, kf, w2), f32),
                pltpu.VMEM((CHUNKS, kf, w1), f32),
                pltpu.VMEM((CHUNKS, kb, rows), bf16),
                pltpu.VMEM((CHUNKS, kb, w2), f32),
                pltpu.VMEM((kb, feats), f32),
                pltpu.VMEM((kb, feats), bf16),
                pltpu.SemaphoreType.DMA((CHUNKS, 40)),
                pltpu.SemaphoreType.DMA((CHUNKS, 40)),
                pltpu.SemaphoreType.DMA((CHUNKS, CORES)),
                pltpu.SemaphoreType.DMA,
                pltpu.SemaphoreType.REGULAR((CHUNKS,)),
            ],
            compiler_params=pltpu.CompilerParams(
                collective_id=0, has_side_effects=True, vmem_limit_bytes=67043328),
        )(design, mine, wt, step_sizes[None, :])
        return w_out[:k].T, r_out[:k].T

    return jax.shard_map(
        local_solve,
        mesh=mesh,
        in_specs=(P('prob', 'feat'), P('prob', None), P(('prob', 'feat'), None), P(('prob', 'feat'))),
        out_specs=(P(('prob', 'feat'), None), P('prob', None)),
        check_vma=False,
    )
```

```python
import functools
import math

import jax
import jax.numpy as jnp
from jax import lax
from jax.experimental import pallas as pl
from jax.experimental.pallas import tpu as pltpu
from jax.sharding import PartitionSpec as P

SWEEPS = 6
RIDGE_COEF = 1.0
MIX_WEIGHT = 0.75
CHUNKS = 4
CORES = 2
SCHEDULE = (
    'A0 A1 B0 B1', 'S0 S1 P0 P1', 'O0 N0 O1 N1', 'a0 a1 A2 A3', 'B2 B3 P2 S2', 'S3 P3 O2 N2', 'O3 N3 p0 p1',
    'o0 o1 s0 s1', 'T0 T1 p2 p3', 'a2 a3 o2 o3', 's2 s3 F0 F1', 'T2 T3 c0 c1', 'F2 F3 e0 e1', 'm0 m1 c2 c3',
    'Q01 H01 G01 n0', 'n1 h01 m2 m3', 'Q23 H23 e2 e3', 'G23 D0 D1 D2', 'D3 n2 n3 h23',
)
MESH = pl.DeviceIdType.MESH


class _Copy:
    def __init__(self, *args):
        self.args = args

    def _make(self):
        src, dst, send_sem, recv_sem, device = self.args
        return pltpu.make_async_remote_copy(src_ref=src, dst_ref=dst, send_sem=send_sem, recv_sem=recv_sem,
                                            device_id=device, device_id_type=MESH)

    def start(self):
        self._make().start()

    def wait_recv(self):
        self._make().wait_recv()

    def wait_send(self):
        self._make().wait_send()


def _up(v, m):
    return (v + m - 1) // m * m


def _split(v, m):
    top = _up(v // 2, m)
    return top, v - top


def _kernel(n, side, kf, kb, x_hbm, y_ref, w0_ref, eta_ref, w_ref, r_hbm,
            xv, c_buf, d_buf, far1, near1, near2, t_buf, rt, own, gacc, dwt,
            send, recv, load_sem, out_sem, free):
    q_all = CHUNKS
    rows = n // q_all
    half = rows // CORES
    w1 = half // side
    w2 = w1 // side
    ka, kc = _split(kf, 8)
    last = SWEEPS

    me = lax.axis_index('feat')
    core = lax.rem(me, CORES)
    px = lax.rem(me // CORES, side)
    py = me // (CORES * side)
    peer = 1 - core
    hbase = pl.multiple_of(core * half, half)
    pbase = pl.multiple_of(peer * half, half)

    def dev(yy, xx, cc):
        return {'feat': (yy * side + xx) * CORES + cc}

    def step(v, s):
        return lax.rem(v + (s + side), side)

    xp, xm = dev(py, step(px, 1), core), dev(py, step(px, -1), core)
    yp, ym = dev(step(py, 1), px, core), dev(step(py, -1), px, core)
    xf, yf = dev(py, step(px, 2), core), dev(step(py, 2), px, core)
    mate = dev(py, px, peer)
    ring_x, ring_y = (px, xp, xm, xf), (py, yp, ym, yf)
    rings = [(ring_x, ring_y) if q % 2 == 0 else (ring_y, ring_x) for q in range(q_all)]

    barrier = pltpu.get_barrier_semaphore()
    for d in (xp, xm, xf, yp, ym, yf, mate):
        pl.semaphore_signal(barrier, inc=1, device_id=d, device_id_type=MESH)

    def load(q, cc):
        def one(i, carry):
            a, b = i // side, lax.rem(i, side)
            d = ((b * side + a) if q % 2 == 0 else (a * side + b)) * CORES + cc
            src = x_hbm.at[pl.ds(pl.multiple_of(d * (q_all * w2) + q * w2, w2), w2), :]
            dst = xv.at[q, pl.ds(pl.multiple_of(cc * half + i * w2, w2), w2), :]
            pltpu.make_async_copy(src, dst, load_sem.at[q, cc]).start()
            return carry
        lax.fori_loop(0, side * side, one, 0)

    def load_wait(q, cc, base):
        ref = xv.at[q, pl.ds(base, half), :]
        pltpu.make_async_copy(ref, ref, load_sem.at[q, cc]).wait()

    for q in range(q_all):
        load(q, peer)
        load(q, core)

    own[...] = y_ref[...]
    gacc[...] = jnp.zeros_like(gacc)
    w_ref[...] = w0_ref[...]
    dwt[...] = w0_ref[...].astype(jnp.bfloat16)
    pl.semaphore_wait(barrier, 7)

    def rc(src, dst, q, k, device):
        return _Copy(src, dst, send.at[q, k], recv.at[q, k], device)

    def lanes(base, width):
        return pl.ds(pl.multiple_of(base, 128), width)

    def blocks(q):
        idx = rings[q][0][0]
        return step(idx, 2), step(idx, 1), step(idx, -1), idx

    def c_d2d(q, j):
        at = blocks(q)[j] * w1
        return rc(c_buf.at[q, :, lanes(pbase + at, w1)], d_buf.at[q, :, lanes(at, w1)], q, j, mate)

    def ring_copies(q):
        idx, plus, minus, _ = rings[q][0]

        def cut(i, lo, size):
            return d_buf.at[q, pl.ds(lo, size), lanes(i * w1, w1)]

        f, p, m = step(idx, 2), step(idx, 1), step(idx, -1)
        return dict(
            far=(rc(cut(f, 0, ka), far1.at[q, 0], q, 4, plus),
                 rc(cut(f, ka, kc), far1.at[q, 1, pl.ds(0, kc), :], q, 5, minus)),
            plain=(rc(cut(p, ka, kc), near1.at[q, 0, pl.ds(ka, kc), :], q, 6, plus),
                   rc(cut(m, 0, ka), near1.at[q, 1, pl.ds(0, ka), :], q, 7, minus)),
            aug=(rc(cut(p, 0, ka), near1.at[q, 0, pl.ds(0, ka), :], q, 8, plus),
                 rc(cut(m, ka, kc), near1.at[q, 1, pl.ds(ka, kc), :], q, 9, minus)))

    def direct_copies(q):
        idx, plus, minus, far = rings[q][1]
        return [rc(t_buf.at[q, :, lanes(step(idx, s) * w2, w2)], near2.at[q, j], q, 10 + j, device)
                for j, (s, device) in enumerate(((2, far), (1, plus), (-1, minus)))]

    def start(copies):
        for c in copies:
            c.start()

    def recv_wait(copies):
        for c in copies:
            c.wait_recv()

    def send_wait(copies):
        for c in copies:
            c.wait_send()

    def ring_mid(q):
        idx = rings[q][0][0]
        cp = ring_copies(q)
        p, m = step(idx, 1), step(idx, -1)
        cp['far'][0].wait_recv()
        at = (q, pl.ds(0, ka), lanes(p * w1, w1))
        d_buf[at] = d_buf[at] + far1[q, 0]
        cp['aug'][0].start()
        cp['far'][1].wait_recv()
        at = (q, pl.ds(ka, kc), lanes(m * w1, w1))
        d_buf[at] = d_buf[at] + far1[q, 1, pl.ds(0, kc), :]
        cp['aug'][1].start()

    def ring_total(q):
        cp = ring_copies(q)
        recv_wait(cp['plain'])
        recv_wait(cp['aug'])
        return d_buf[q, :, lanes(rings[q][0][0] * w1, w1)] + (near1[q, 0] + near1[q, 1])

    def direct_total(q):
        recv_wait(direct_copies(q))
        return t_buf[q, :, lanes(rings[q][1][0] * w2, w2)] + near2[q, 0] + (near2[q, 1] + near2[q, 2])

    def ag_copies(q, wide):
        (i1, p1, m1, o1), (i2, p2, m2, o2) = rings[q]
        buf = c_buf if wide else rt
        b0 = hbase + i1 * w1

        def to(base, width, k, device):
            ref = buf.at[q, :, lanes(base, width)]
            return rc(ref, ref, q, k, device)

        pieces = [b0 + step(i2, s) * w2 for s in (0, -1, 1, 2)]
        return dict(
            n1=[to(pieces[0], w2, 13 + j, device) for j, device in enumerate((p2, m2, o2))],
            n2=[[to(at, w2, 16 + 3 * i + j, device) for j, device in enumerate((p1, m1, o1))]
                for i, at in enumerate(pieces)],
            x=[to(hbase + step(i1, s) * w1, w1, 28 + j, mate) for j, s in enumerate((0, -1, 1, 2))])

    def ag_first(q, wide):
        cp = ag_copies(q, wide)
        start(cp['n1'])
        start(cp['n2'][0])

    def ag_second(q, wide):
        cp = ag_copies(q, wide)
        for j in range(3):
            cp['n1'][j].wait_recv()
            start(cp['n2'][1 + j])
        if wide:
            pl.semaphore_wait(free.at[q], 1)
        cp['x'][0].start()

    def ag_third(q, wide):
        cp = ag_copies(q, wide)
        for j in range(3):
            for i in range(4):
                cp['n2'][i][j].wait_recv()
            cp['x'][1 + j].start()

    def ag_mate(q, wide):
        ag_copies(q, wide)['x'][0].wait_recv()

    def ag_mate2(q, wide):
        recv_wait(ag_copies(q, wide)['x'][1:])

    def partial_product(q, base, js):
        for j in js:
            at = pl.ds(pl.multiple_of(base + blocks(q)[j] * w1, w1), w1)
            v = lax.dot_general(dwt[...], xv[q, at, :], (((1,), (1,)), ((), ())), preferred_element_type=jnp.float32)
            c_buf[q, :, at] = v[:kf]

    def gradient(parts):
        total = None
        for q, base, j in parts:
            at = pl.ds(pl.multiple_of(base + blocks(q)[j] * w1, w1), w1)
            v = jnp.dot(rt[q, :, at], xv[q, at, :], preferred_element_type=jnp.float32)
            total = v if total is None else total + v
        gacc[...] += total

    def sweep(t, carry):
        first = t == 0
        scale = jnp.where(first, jnp.float32(1.0), jnp.float32(MIX_WEIGHT))

        def gathers(f, q):
            @pl.when(t < last)
            def _():
                f(q, False)

            @pl.when(t == last)
            def _():
                f(q, True)

        def product(q, mates, js, opens=False):
            if opens:
                @pl.when(first)
                def _():
                    load_wait(q, peer, pbase)
                    load_wait(q, core, hbase)
            partial_product(q, pbase if mates else hbase, js)
            if mates:
                start([c_d2d(q, j) for j in js])

        def pair_sum(q, js, then):
            for j in js:
                c_d2d(q, j).wait_recv()
                at = blocks(q)[j] * w1
                d_buf[q, :, lanes(at, w1)] = d_buf[q, :, lanes(at, w1)] + c_buf[q, :, lanes(hbase + at, w1)]
            if then:
                start(ring_copies(q)[then])

        def ring_sum(q):
            t_buf[q] = ring_total(q)
            start(direct_copies(q))
            send_wait([c_d2d(q, j) for j in range(4)])

            @pl.when(t == last)
            def _():
                pl.semaphore_signal(free.at[q], inc=1, device_id=mate, device_id_type=MESH)

        def finish(q):
            fresh = own[q, pl.ds(0, kf), :] - scale * direct_total(q)
            own[q, pl.ds(0, kf), :] = fresh
            for copies in ring_copies(q).values():
                send_wait(copies)
            idx = rings[q]
            at = lanes(hbase + idx[0][0] * w1 + idx[1][0] * w2, w2)

            @pl.when(t < last)
            def _():
                rt[q, :, at] = own[q].astype(jnp.bfloat16)

            @pl.when(t == last)
            def _():
                c_buf[q, :, at] = own[q, pl.ds(0, kf), :]
            gathers(ag_first, q)

        def grad(qs, base, js):
            @pl.when(t < last)
            def _():
                gradient([(q, base, j) for q in qs for j in js])

        def drain(q, wide):
            cp = ag_copies(q, wide)
            for copies in [cp['n1'], cp['x']] + cp['n2']:
                send_wait(copies)

        def drained(q):
            send_wait(direct_copies(q))
            gathers(drain, q)

        def each(f):
            return lambda qs: [f(q) for q in qs]

        acts = {
            'A': each(lambda q: product(q, True, (0,), True)), 'B': each(lambda q: product(q, False, (0,))),
            'P': each(lambda q: product(q, True, (1, 2))), 'O': each(lambda q: product(q, False, (1, 2))),
            'p': each(lambda q: product(q, True, (3,))), 'o': each(lambda q: product(q, False, (3,))),
            'S': each(lambda q: pair_sum(q, (0,), 'far')), 'N': each(lambda q: pair_sum(q, (1, 2), 'plain')),
            's': each(lambda q: pair_sum(q, (3,), None)),
            'a': each(ring_mid), 'T': each(ring_sum), 'F': each(finish),
            'c': each(lambda q: gathers(ag_second, q)), 'e': each(lambda q: gathers(ag_third, q)),
            'm': each(lambda q: gathers(ag_mate, q)), 'n': each(lambda q: gathers(ag_mate2, q)),
            'Q': lambda qs: grad(qs, hbase, (3,)), 'G': lambda qs: grad(qs, hbase, (0, 1, 2)),
            'H': lambda qs: grad(qs, pbase, (3,)), 'h': lambda qs: grad(qs, pbase, (0, 1, 2)),
            'D': each(drained),
        }
        for act in ' '.join(SCHEDULE).split():
            with jax.named_scope(act):
                acts[act[0]]([int(v) for v in act[1:]])

        @pl.when(t < last)
        def _():
            update = eta_ref[...] * (gacc[...] * (1.0 / n) - (RIDGE_COEF / n) * w_ref[...])
            w_ref[...] = w_ref[...] + MIX_WEIGHT * update
            dwt[...] = update.astype(jnp.bfloat16)
            gacc[...] = jnp.zeros_like(gacc)
        return carry

    lax.fori_loop(0, last + 1, sweep, 0)

    def piece(i, carry):
        for q in range(q_all):
            cc, j = i // (side * side), lax.rem(i, side * side)
            a, b = j // side, lax.rem(j, side)
            d = ((b * side + a) if q % 2 == 0 else (a * side + b)) * CORES + cc
            pltpu.make_async_copy(c_buf.at[q, :, lanes(i * w2, w2)],
                                  r_hbm.at[:, lanes((d * q_all + q) * w2, w2)], out_sem).start()
        return carry
    lax.fori_loop(0, CORES * side * side, piece, 0)
    for q in range(q_all):
        pltpu.make_async_copy(c_buf.at[q], c_buf.at[q], out_sem).wait()


def solution(mesh):
    group = mesh.shape['feat']
    side = math.isqrt(group // CORES)

    def local_solve(design, targets, weights, step_sizes):
        n, feats = design.shape
        k = targets.shape[1]
        kf, kb = _up(k, 8), _up(k, 16)
        rows = n // CHUNKS
        half = rows // CORES
        w1 = half // side
        w2 = w1 // side
        ka = _split(kf, 8)[0]
        share = n // group
        me = lax.axis_index('feat')
        mine = lax.dynamic_slice_in_dim(targets, me * share, share, 0)
        mine = jnp.pad(jnp.swapaxes(mine.reshape(CHUNKS, w2, k), 1, 2), ((0, 0), (0, kb - k), (0, 0)))
        wt = jnp.pad(weights.T, ((0, kb - k), (0, 0)))
        f32, bf16 = jnp.float32, jnp.bfloat16
        vm = pl.BlockSpec(memory_space=pltpu.VMEM)
        hb = pl.BlockSpec(memory_space=pl.ANY)
        w_out, r_out = pl.pallas_call(
            functools.partial(_kernel, n, side, kf, kb),
            out_shape=(jax.ShapeDtypeStruct((kb, feats), f32), jax.ShapeDtypeStruct((kf, n), f32)),
            in_specs=[hb, vm, vm, vm],
            out_specs=(vm, hb),
            scratch_shapes=[
                pltpu.VMEM((CHUNKS, rows, feats), bf16),
                pltpu.VMEM((CHUNKS, kf, rows), f32),
                pltpu.VMEM((CHUNKS, kf, half), f32),
                pltpu.VMEM((CHUNKS, 2, ka, w1), f32),
                pltpu.VMEM((CHUNKS, 2, kf, w1), f32),
                pltpu.VMEM((CHUNKS, 3, kf, w2), f32),
                pltpu.VMEM((CHUNKS, kf, w1), f32),
                pltpu.VMEM((CHUNKS, kb, rows), bf16),
                pltpu.VMEM((CHUNKS, kb, w2), f32),
                pltpu.VMEM((kb, feats), f32),
                pltpu.VMEM((kb, feats), bf16),
                pltpu.SemaphoreType.DMA((CHUNKS, 32)),
                pltpu.SemaphoreType.DMA((CHUNKS, 32)),
                pltpu.SemaphoreType.DMA((CHUNKS, CORES)),
                pltpu.SemaphoreType.DMA,
                pltpu.SemaphoreType.REGULAR((CHUNKS,)),
            ],
            compiler_params=pltpu.CompilerParams(
                collective_id=0, has_side_effects=True, vmem_limit_bytes=67043328),
        )(design, mine, wt, step_sizes[None, :])
        return w_out[:k].T, r_out[:k].T

    return jax.shard_map(
        local_solve,
        mesh=mesh,
        in_specs=(P('prob', 'feat'), P('prob', None), P(('prob', 'feat'), None), P(('prob', 'feat'))),
        out_specs=(P(('prob', 'feat'), None), P('prob', None)),
        check_vma=False,
    )
```

```python
import functools
import math

import jax
import jax.numpy as jnp
from jax import lax
from jax.experimental import pallas as pl
from jax.experimental.pallas import tpu as pltpu
from jax.sharding import PartitionSpec as P

SWEEPS = 6
RIDGE_COEF = 1.0
MIX_WEIGHT = 0.75
CHUNKS = 4
CORES = 2
SCHEDULE = (
    'A0 A1 B0 B1', 'S0 S1 P0 P1', 'O0 N0 O1 N1', 'a0 a1 A2 A3', 'B2 B3 P2 S2', 'S3 P3 O2 N2', 'O3 N3 p0 p1',
    'o0 o1 s0 s1', 'T0 T1 p2 p3', 'a2 a3 o2 o3', 's2 s3 F0 F1', 'T2 T3 c0 c1', 'F2 F3 e0 e1', 'm0 m1 c2 c3',
    'Q01 H01 G01 n0', 'n1 R0 R1 h01', 'm2 m3 Q23 H23', 'e2 e3 G23 D0', 'D1 D2 D3 n2', 'n3 R2 R3 h23',
)
MESH = pl.DeviceIdType.MESH


class _Copy:
    def __init__(self, *args):
        self.args = args

    def _make(self):
        src, dst, send_sem, recv_sem, device = self.args
        return pltpu.make_async_remote_copy(src_ref=src, dst_ref=dst, send_sem=send_sem, recv_sem=recv_sem,
                                            device_id=device, device_id_type=MESH)

    def start(self):
        self._make().start()

    def wait_recv(self):
        self._make().wait_recv()

    def wait_send(self):
        self._make().wait_send()


def _kernel(n, side, x_hbm, y_hbm, w0_ref, eta_ref, w_ref, r_hbm,
            xv, c_buf, d_buf, far1, near1, near2, t_buf, rt, own, gacc, dwt, y_own,
            send, recv, load_sem, out_sem, free):
    q_all = CHUNKS
    rows = n // q_all
    half = rows // CORES
    w1 = half // side
    w2 = w1 // side
    wh = w1 // 2
    share = q_all * w2
    last = SWEEPS

    me = lax.axis_index('feat')
    core = lax.rem(me, CORES)
    px = lax.rem(me // CORES, side)
    py = me // (CORES * side)
    peer = 1 - core
    hbase = pl.multiple_of(core * half, half)
    pbase = pl.multiple_of(peer * half, half)

    def dev(yy, xx, cc):
        return {'feat': (yy * side + xx) * CORES + cc}

    def step(v, s):
        return lax.rem(v + (s + side), side)

    xp, xm = dev(py, step(px, 1), core), dev(py, step(px, -1), core)
    yp, ym = dev(step(py, 1), px, core), dev(step(py, -1), px, core)
    xf, yf = dev(py, step(px, 2), core), dev(step(py, 2), px, core)
    mate = dev(py, px, peer)
    ring_x, ring_y = (px, xp, xm, xf), (py, yp, ym, yf)
    rings = [(ring_x, ring_y) if q % 2 == 0 else (ring_y, ring_x) for q in range(q_all)]

    barrier = pltpu.get_barrier_semaphore()
    for d in (xp, xm, xf, yp, ym, yf, mate):
        pl.semaphore_signal(barrier, inc=1, device_id=d, device_id_type=MESH)

    def load(q, cc):
        def one(i, carry):
            a, b = i // side, lax.rem(i, side)
            d = ((b * side + a) if q % 2 == 0 else (a * side + b)) * CORES + cc
            src = x_hbm.at[pl.ds(pl.multiple_of(d * (q_all * w2) + q * w2, w2), w2), :]
            dst = xv.at[q, pl.ds(pl.multiple_of(cc * half + i * w2, w2), w2), :]
            pltpu.make_async_copy(src, dst, load_sem.at[q, cc]).start()
            return carry
        lax.fori_loop(0, side * side, one, 0)

    def load_wait(q, cc, base):
        ref = xv.at[q, pl.ds(base, half), :]
        pltpu.make_async_copy(ref, ref, load_sem.at[q, cc]).wait()

    targets_in = pltpu.make_async_copy(y_hbm.at[:, pl.ds(pl.multiple_of(me * share, share), share)], y_own, out_sem)
    targets_in.start()
    for q in range(q_all):
        load(q, peer)
        load(q, core)

    gacc[...] = jnp.zeros_like(gacc)
    w_ref[...] = w0_ref[...]
    dwt[...] = w0_ref[...].astype(jnp.bfloat16)
    targets_in.wait()
    for q in range(q_all):
        own[q] = y_own[:, q * w2:(q + 1) * w2]
    pl.semaphore_wait(barrier, 7)

    def rc(src, dst, q, k, device):
        return _Copy(src, dst, send.at[q, k], recv.at[q, k], device)

    def lanes(base, width):
        return pl.ds(pl.multiple_of(base, 128), width)

    def blocks(q):
        idx = rings[q][0][0]
        return step(idx, 2), step(idx, 1), step(idx, -1), idx

    def c_d2d(q, j):
        at = blocks(q)[j] * w1
        return rc(c_buf.at[q, :, lanes(pbase + at, w1)], d_buf.at[q, :, lanes(at, w1)], q, j, mate)

    def ring_copies(q):
        idx, plus, minus, _ = rings[q][0]

        def cut(i, side_half):
            return d_buf.at[q, :, lanes(i * w1 + side_half * wh, wh)]

        def into(j, side_half):
            return near1.at[q, j, :, pl.ds(side_half * wh, wh)]

        f, p, m = step(idx, 2), step(idx, 1), step(idx, -1)
        return dict(
            far=(rc(cut(f, 0), far1.at[q, 0], q, 4, plus), rc(cut(f, 1), far1.at[q, 1], q, 5, minus)),
            plain=(rc(cut(p, 1), into(0, 1), q, 6, plus), rc(cut(m, 0), into(1, 0), q, 7, minus)),
            aug=(rc(cut(p, 0), into(0, 0), q, 8, plus), rc(cut(m, 1), into(1, 1), q, 9, minus)))

    def direct_copies(q):
        idx, plus, minus, far = rings[q][1]
        return [rc(t_buf.at[q, :, lanes(step(idx, s) * w2, w2)], near2.at[q, j], q, 10 + j, device)
                for j, (s, device) in enumerate(((2, far), (1, plus), (-1, minus)))]

    def start(copies):
        for c in copies:
            c.start()

    def recv_wait(copies):
        for c in copies:
            c.wait_recv()

    def send_wait(copies):
        for c in copies:
            c.wait_send()

    def ring_mid(q):
        idx = rings[q][0][0]
        cp = ring_copies(q)
        p, m = step(idx, 1), step(idx, -1)
        for j, i in enumerate((p, m)):
            cp['far'][j].wait_recv()
            at = (q, slice(None), lanes(i * w1 + j * wh, wh))
            d_buf[at] = d_buf[at] + far1[q, j]
            cp['aug'][j].start()

    def ring_total(q):
        cp = ring_copies(q)
        recv_wait(cp['plain'])
        recv_wait(cp['aug'])
        return d_buf[q, :, lanes(rings[q][0][0] * w1, w1)] + (near1[q, 0] + near1[q, 1])

    def direct_total(q):
        recv_wait(direct_copies(q))
        return t_buf[q, :, lanes(rings[q][1][0] * w2, w2)] + near2[q, 0] + (near2[q, 1] + near2[q, 2])

    def ag_copies(q, wide):
        (i1, p1, m1, o1), (i2, p2, m2, o2) = rings[q]
        buf = c_buf if wide else rt
        b0 = hbase + i1 * w1

        def to(base, width, k, device):
            ref = buf.at[q, :, lanes(base, width)]
            return rc(ref, ref, q, k, device)

        pieces = [b0 + step(i2, s) * w2 for s in (0, -1, 1, 2)]
        return dict(
            n1=[to(pieces[0], w2, 13 + j, device) for j, device in enumerate((p2, m2, o2))],
            n2=[[to(at, w2, 16 + 3 * i + j, device) for j, device in enumerate((p1, m1, o1))]
                for i, at in enumerate(pieces)],
            x=[to(hbase + step(i1, s) * w1, w1, 28 + j, mate) for j, s in enumerate((0, -1, 1, 2))])

    def ag_first(q, wide):
        cp = ag_copies(q, wide)
        start(cp['n1'])
        start(cp['n2'][0])

    def ag_second(q, wide):
        cp = ag_copies(q, wide)
        for j in range(3):
            cp['n1'][j].wait_recv()
            start(cp['n2'][1 + j])
        if wide:
            pl.semaphore_wait(free.at[q], 1)
        cp['x'][0].start()

    def ag_third(q, wide):
        cp = ag_copies(q, wide)
        for j in range(3):
            for i in range(4):
                cp['n2'][i][j].wait_recv()
            cp['x'][1 + j].start()

    def ag_mate(q, wide):
        ag_copies(q, wide)['x'][0].wait_recv()

    def ag_mate2(q, wide):
        recv_wait(ag_copies(q, wide)['x'][1:])

    def partial_product(q, base, js):
        for j in js:
            at = pl.ds(pl.multiple_of(base + blocks(q)[j] * w1, w1), w1)
            v = lax.dot_general(dwt[...], xv[q, at, :], (((1,), (1,)), ((), ())), preferred_element_type=jnp.float32)
            c_buf[q, :, at] = v

    def gradient(parts):
        total = None
        for q, base, j in parts:
            at = pl.ds(pl.multiple_of(base + blocks(q)[j] * w1, w1), w1)
            v = jnp.dot(rt[q, :, at], xv[q, at, :], preferred_element_type=jnp.float32)
            total = v if total is None else total + v
        gacc[...] += total

    def sweep(t, carry):
        first = t == 0
        scale = jnp.where(first, jnp.float32(1.0), jnp.float32(MIX_WEIGHT))

        def gathers(f, q):
            @pl.when(t < last)
            def _():
                f(q, False)

            @pl.when(t == last)
            def _():
                f(q, True)

        def product(q, mates, js, opens=False):
            if opens:
                @pl.when(first)
                def _():
                    load_wait(q, peer, pbase)
                    load_wait(q, core, hbase)
            partial_product(q, pbase if mates else hbase, js)
            if mates:
                start([c_d2d(q, j) for j in js])

        def pair_sum(q, js, then):
            for j in js:
                c_d2d(q, j).wait_recv()
                at = blocks(q)[j] * w1
                d_buf[q, :, lanes(at, w1)] = d_buf[q, :, lanes(at, w1)] + c_buf[q, :, lanes(hbase + at, w1)]
            if then:
                start(ring_copies(q)[then])

        def ring_sum(q):
            t_buf[q] = ring_total(q)
            start(direct_copies(q))
            send_wait([c_d2d(q, j) for j in range(4)])

            @pl.when(t == last)
            def _():
                pl.semaphore_signal(free.at[q], inc=1, device_id=mate, device_id_type=MESH)

        def finish(q):
            fresh = own[q] - scale * direct_total(q)
            own[q] = fresh
            for copies in ring_copies(q).values():
                send_wait(copies)
            idx = rings[q]
            at = lanes(hbase + idx[0][0] * w1 + idx[1][0] * w2, w2)

            @pl.when(t < last)
            def _():
                rt[q, :, at] = own[q].astype(jnp.bfloat16)

            @pl.when(t == last)
            def _():
                c_buf[q, :, at] = own[q]
            gathers(ag_first, q)

        def grad(qs, base, js):
            @pl.when(t < last)
            def _():
                gradient([(q, base, j) for q in qs for j in js])

        def drain(q, wide):
            cp = ag_copies(q, wide)
            for copies in [cp['n1'], cp['x']] + cp['n2']:
                send_wait(copies)

        def drained(q):
            send_wait(direct_copies(q))
            gathers(drain, q)

        def put(q):
            def piece(i, carry):
                cc, j = i // (side * side), lax.rem(i, side * side)
                a, b = j // side, lax.rem(j, side)
                d = ((b * side + a) if q % 2 == 0 else (a * side + b)) * CORES + cc
                pltpu.make_async_copy(c_buf.at[q, :, lanes(i * w2, w2)],
                                      r_hbm.at[:, lanes((d * q_all + q) * w2, w2)], out_sem).start()
                return carry

            @pl.when(t == last)
            def _():
                lax.fori_loop(0, CORES * side * side, piece, 0)

        def each(f):
            return lambda qs: [f(q) for q in qs]

        acts = {
            'A': each(lambda q: product(q, True, (0,), True)), 'B': each(lambda q: product(q, False, (0,))),
            'P': each(lambda q: product(q, True, (1, 2))), 'O': each(lambda q: product(q, False, (1, 2))),
            'p': each(lambda q: product(q, True, (3,))), 'o': each(lambda q: product(q, False, (3,))),
            'S': each(lambda q: pair_sum(q, (0,), 'far')), 'N': each(lambda q: pair_sum(q, (1, 2), 'plain')),
            's': each(lambda q: pair_sum(q, (3,), None)),
            'a': each(ring_mid), 'T': each(ring_sum), 'F': each(finish),
            'c': each(lambda q: gathers(ag_second, q)), 'e': each(lambda q: gathers(ag_third, q)),
            'm': each(lambda q: gathers(ag_mate, q)), 'n': each(lambda q: gathers(ag_mate2, q)),
            'Q': lambda qs: grad(qs, hbase, (3,)), 'G': lambda qs: grad(qs, hbase, (0, 1, 2)),
            'H': lambda qs: grad(qs, pbase, (3,)), 'h': lambda qs: grad(qs, pbase, (0, 1, 2)),
            'D': each(drained), 'R': each(put),
        }
        for act in ' '.join(SCHEDULE).split():
            with jax.named_scope(act):
                acts[act[0]]([int(v) for v in act[1:]])

        @pl.when(t < last)
        def _():
            update = eta_ref[...] * (gacc[...] * (1.0 / n) - (RIDGE_COEF / n) * w_ref[...])
            w_ref[...] = w_ref[...] + MIX_WEIGHT * update
            dwt[...] = update.astype(jnp.bfloat16)
            gacc[...] = jnp.zeros_like(gacc)
        return carry

    lax.fori_loop(0, last + 1, sweep, 0)

    for q in range(q_all):
        pltpu.make_async_copy(c_buf.at[q], c_buf.at[q], out_sem).wait()


def solution(mesh):
    group = mesh.shape['feat']
    side = math.isqrt(group // CORES)

    def local_solve(design, targets, weights, step_sizes):
        n, feats = design.shape
        k = targets.shape[1]
        rows = n // CHUNKS
        half = rows // CORES
        w1 = half // side
        w2 = w1 // side
        f32, bf16 = jnp.float32, jnp.bfloat16
        vm = pl.BlockSpec(memory_space=pltpu.VMEM)
        hb = pl.BlockSpec(memory_space=pl.ANY)
        w_out, r_out = pl.pallas_call(
            functools.partial(_kernel, n, side),
            out_shape=(jax.ShapeDtypeStruct((k, feats), f32), jax.ShapeDtypeStruct((k, n), f32)),
            in_specs=[hb, hb, vm, vm],
            out_specs=(vm, hb),
            scratch_shapes=[
                pltpu.VMEM((CHUNKS, rows, feats), bf16),
                pltpu.VMEM((CHUNKS, k, rows), f32),
                pltpu.VMEM((CHUNKS, k, half), f32),
                pltpu.VMEM((CHUNKS, 2, k, w1 // 2), f32),
                pltpu.VMEM((CHUNKS, 2, k, w1), f32),
                pltpu.VMEM((CHUNKS, 3, k, w2), f32),
                pltpu.VMEM((CHUNKS, k, w1), f32),
                pltpu.VMEM((CHUNKS, k, rows), bf16),
                pltpu.VMEM((CHUNKS, k, w2), f32),
                pltpu.VMEM((k, feats), f32),
                pltpu.VMEM((k, feats), bf16),
                pltpu.VMEM((k, CHUNKS * w2), f32),
                pltpu.SemaphoreType.DMA((CHUNKS, 32)),
                pltpu.SemaphoreType.DMA((CHUNKS, 32)),
                pltpu.SemaphoreType.DMA((CHUNKS, CORES)),
                pltpu.SemaphoreType.DMA,
                pltpu.SemaphoreType.REGULAR((CHUNKS,)),
            ],
            compiler_params=pltpu.CompilerParams(
                collective_id=0, has_side_effects=True, vmem_limit_bytes=67043328),
        )(design, targets.T, weights.T, step_sizes[None, :])
        return w_out.T, r_out.T

    return jax.shard_map(
        local_solve,
        mesh=mesh,
        in_specs=(P('prob', 'feat'), P('prob', None), P(('prob', 'feat'), None), P(('prob', 'feat'))),
        out_specs=(P(('prob', 'feat'), None), P('prob', None)),
        check_vma=False,
    )
```

```python
import functools
import math

import jax
import jax.numpy as jnp
from jax import lax
from jax.experimental import pallas as pl
from jax.experimental.pallas import tpu as pltpu
from jax.sharding import PartitionSpec as P

SWEEPS = 6
RIDGE_COEF = 1.0
MIX_WEIGHT = 0.75
CHUNKS = 4
CORES = 2
PARTS = 8
SCHEDULE = (
    'A0 A1 B0 B1', 'S0 S1 P0 P1', 'O0 N0 O1 N1', 'a0 a1 A2 A3', 'B2 B3 P2 S2', 'S3 P3 O2 N2', 'O3 N3 p0 p1',
    'o0 o1 s0 s1', 'T0 T1 p2 p3', 'a2 a3 o2 o3', 's2 s3 F0 F1', 'T2 T3 c0 c1', 'F2 F3 e0 e1', 'm0 m1 c2 c3',
    'Q01 H01 G01 n0', 'n1 R0 R1 h01', 'm2 m3 Q23 H23', 'e2 e3 G23 D0', 'D1 D2 D3 n2', 'n3 R2 R3 h23',
)
MESH = pl.DeviceIdType.MESH


class _Copy:
    def __init__(self, *args):
        self.args = args

    def _make(self):
        src, dst, send_sem, recv_sem, device = self.args
        return pltpu.make_async_remote_copy(src_ref=src, dst_ref=dst, send_sem=send_sem, recv_sem=recv_sem,
                                            device_id=device, device_id_type=MESH)

    def start(self):
        self._make().start()

    def wait_recv(self):
        self._make().wait_recv()

    def wait_send(self):
        self._make().wait_send()


def _kernel(n, side, x_hbm, y_hbm, w0_ref, eta_ref, w_ref, r_hbm,
            xv, c_buf, d_buf, far1, near1, near2, t_buf, rt, own, gacc, dwt, y_own,
            send, recv, load_sem, out_sem, free):
    q_all = CHUNKS
    rows = n // q_all
    half = rows // CORES
    w1 = half // side
    w2 = w1 // side
    wh = w1 // 2
    share = q_all * w2
    last = SWEEPS

    me = lax.axis_index('feat')
    core = lax.rem(me, CORES)
    px = lax.rem(me // CORES, side)
    py = me // (CORES * side)
    peer = 1 - core
    hbase = pl.multiple_of(core * half, half)
    pbase = pl.multiple_of(peer * half, half)

    def dev(yy, xx, cc):
        return {'feat': (yy * side + xx) * CORES + cc}

    def step(v, s):
        return lax.rem(v + (s + side), side)

    xp, xm = dev(py, step(px, 1), core), dev(py, step(px, -1), core)
    yp, ym = dev(step(py, 1), px, core), dev(step(py, -1), px, core)
    xf, yf = dev(py, step(px, 2), core), dev(step(py, 2), px, core)
    mate = dev(py, px, peer)
    ring_x, ring_y = (px, xp, xm, xf), (py, yp, ym, yf)
    rings = [(ring_x, ring_y) if q % 2 == 0 else (ring_y, ring_x) for q in range(q_all)]

    barrier = pltpu.get_barrier_semaphore()
    for d in (xp, xm, xf, yp, ym, yf, mate):
        pl.semaphore_signal(barrier, inc=1, device_id=d, device_id_type=MESH)

    def blocks(q):
        idx = rings[q][0][0]
        return step(idx, 2), step(idx, 1), step(idx, -1), idx

    def load(q, cc, j):
        a = blocks(q)[j]

        def one(b, carry):
            d = ((b * side + a) if q % 2 == 0 else (a * side + b)) * CORES + cc
            src = x_hbm.at[pl.ds(pl.multiple_of(d * share + q * w2, w2), w2), :]
            dst = xv.at[q, pl.ds(pl.multiple_of(cc * half + a * w1 + b * w2, w2), w2), :]
            pltpu.make_async_copy(src, dst, load_sem.at[q, cc, j]).start()
            return carry
        lax.fori_loop(0, side, one, 0)

    def load_wait(q, js):
        for cc in (peer, core):
            for j in js:
                ref = xv.at[q, pl.ds(pl.multiple_of(cc * half + blocks(q)[j] * w1, w1), w1), :]
                pltpu.make_async_copy(ref, ref, load_sem.at[q, cc, j]).wait()

    targets_in = pltpu.make_async_copy(y_hbm.at[:, pl.ds(pl.multiple_of(me * share, share), share)], y_own, out_sem)
    targets_in.start()
    for qs in ((0, 1), (2, 3)):
        for js in ((0,), (1, 2), (3,)):
            for q in qs:
                for cc in (peer, core):
                    for j in js:
                        load(q, cc, j)

    gacc[...] = jnp.zeros_like(gacc)
    w_ref[...] = w0_ref[...]
    dwt[...] = w0_ref[...].astype(jnp.bfloat16)
    targets_in.wait()
    for q in range(q_all):
        own[q] = y_own[:, q * w2:(q + 1) * w2]
    pl.semaphore_wait(barrier, 7)

    def rc(src, dst, q, k, device):
        return _Copy(src, dst, send.at[q, k], recv.at[q, k], device)

    def lanes(base, width):
        return pl.ds(pl.multiple_of(base, 128), width)

    def c_d2d(q, j):
        at = blocks(q)[j] * w1
        return rc(c_buf.at[q, :, lanes(pbase + at, w1)], d_buf.at[q, :, lanes(at, w1)], q, j, mate)

    def ring_copies(q):
        idx, plus, minus, _ = rings[q][0]

        def cut(i, side_half):
            return d_buf.at[q, :, lanes(i * w1 + side_half * wh, wh)]

        def into(j, side_half):
            return near1.at[q, j, :, pl.ds(side_half * wh, wh)]

        f, p, m = step(idx, 2), step(idx, 1), step(idx, -1)
        return dict(
            far=(rc(cut(f, 0), far1.at[q, 0], q, 4, plus), rc(cut(f, 1), far1.at[q, 1], q, 5, minus)),
            plain=(rc(cut(p, 1), into(0, 1), q, 6, plus), rc(cut(m, 0), into(1, 0), q, 7, minus)),
            aug=(rc(cut(p, 0), into(0, 0), q, 8, plus), rc(cut(m, 1), into(1, 1), q, 9, minus)))

    def direct_copies(q):
        idx, plus, minus, far = rings[q][1]
        return [rc(t_buf.at[q, :, lanes(step(idx, s) * w2, w2)], near2.at[q, j], q, 10 + j, device)
                for j, (s, device) in enumerate(((2, far), (1, plus), (-1, minus)))]

    def start(copies):
        for c in copies:
            c.start()

    def recv_wait(copies):
        for c in copies:
            c.wait_recv()

    def send_wait(copies):
        for c in copies:
            c.wait_send()

    def ring_mid(q):
        idx = rings[q][0][0]
        cp = ring_copies(q)
        p, m = step(idx, 1), step(idx, -1)
        for j, i in enumerate((p, m)):
            cp['far'][j].wait_recv()
            at = (q, slice(None), lanes(i * w1 + j * wh, wh))
            d_buf[at] = d_buf[at] + far1[q, j]
            cp['aug'][j].start()

    def ring_total(q):
        cp = ring_copies(q)
        recv_wait(cp['plain'])
        recv_wait(cp['aug'])
        return d_buf[q, :, lanes(rings[q][0][0] * w1, w1)] + (near1[q, 0] + near1[q, 1])

    def direct_total(q):
        recv_wait(direct_copies(q))
        return t_buf[q, :, lanes(rings[q][1][0] * w2, w2)] + near2[q, 0] + (near2[q, 1] + near2[q, 2])

    def ag_copies(q, wide):
        (i1, p1, m1, o1), (i2, p2, m2, o2) = rings[q]
        buf = c_buf if wide else rt
        b0 = hbase + i1 * w1

        def to(base, width, k, device):
            ref = buf.at[q, :, lanes(base, width)]
            return rc(ref, ref, q, k, device)

        pieces = [b0 + step(i2, s) * w2 for s in (0, -1, 1, 2)]
        return dict(
            n1=[to(pieces[0], w2, 13 + j, device) for j, device in enumerate((p2, m2, o2))],
            n2=[[to(at, w2, 16 + 3 * i + j, device) for j, device in enumerate((p1, m1, o1))]
                for i, at in enumerate(pieces)],
            x=[to(hbase + step(i1, s) * w1, w1, 28 + j, mate) for j, s in enumerate((0, -1, 1, 2))])

    def ag_first(q, wide):
        cp = ag_copies(q, wide)
        start(cp['n1'])
        start(cp['n2'][0])

    def ag_second(q, wide):
        cp = ag_copies(q, wide)
        for j in range(3):
            cp['n1'][j].wait_recv()
            start(cp['n2'][1 + j])
        if wide:
            pl.semaphore_wait(free.at[q], 1)
        cp['x'][0].start()

    def ag_third(q, wide):
        cp = ag_copies(q, wide)
        for j in range(3):
            for i in range(4):
                cp['n2'][i][j].wait_recv()
            cp['x'][1 + j].start()

    def ag_mate(q, wide):
        ag_copies(q, wide)['x'][0].wait_recv()

    def ag_mate2(q, wide):
        recv_wait(ag_copies(q, wide)['x'][1:])

    def partial_product(q, base, js):
        for j in js:
            at = pl.ds(pl.multiple_of(base + blocks(q)[j] * w1, w1), w1)
            v = lax.dot_general(dwt[...], xv[q, at, :], (((1,), (1,)), ((), ())), preferred_element_type=jnp.float32)
            c_buf[q, :, at] = v

    def gradient(parts):
        total = None
        for q, base, j in parts:
            at = pl.ds(pl.multiple_of(base + blocks(q)[j] * w1, w1), w1)
            v = jnp.dot(rt[q, :, at], xv[q, at, :], preferred_element_type=jnp.float32)
            total = v if total is None else total + v
        gacc[...] += total

    def sweep(t, carry):
        first = t == 0
        scale = jnp.where(first, jnp.float32(1.0), jnp.float32(MIX_WEIGHT))

        def gathers(f, q):
            @pl.when(t < last)
            def _():
                f(q, False)

            @pl.when(t == last)
            def _():
                f(q, True)

        def product(q, mates, js):
            if mates and (q < 2 or 0 in js):
                @pl.when(first)
                def _():
                    load_wait(q, js if q < 2 else range(4))
            partial_product(q, pbase if mates else hbase, js)
            if mates:
                start([c_d2d(q, j) for j in js])

        def pair_sum(q, js, then):
            for j in js:
                c_d2d(q, j).wait_recv()
                at = blocks(q)[j] * w1
                d_buf[q, :, lanes(at, w1)] = d_buf[q, :, lanes(at, w1)] + c_buf[q, :, lanes(hbase + at, w1)]
            if then:
                start(ring_copies(q)[then])

        def ring_sum(q):
            t_buf[q] = ring_total(q)
            start(direct_copies(q))
            send_wait([c_d2d(q, j) for j in range(4)])

            @pl.when(t == last)
            def _():
                pl.semaphore_signal(free.at[q], inc=1, device_id=mate, device_id_type=MESH)

        def finish(q):
            fresh = own[q] - scale * direct_total(q)
            own[q] = fresh
            for copies in ring_copies(q).values():
                send_wait(copies)
            idx = rings[q]
            at = lanes(hbase + idx[0][0] * w1 + idx[1][0] * w2, w2)

            @pl.when(t < last)
            def _():
                rt[q, :, at] = own[q].astype(jnp.bfloat16)

            @pl.when(t == last)
            def _():
                c_buf[q, :, at] = own[q]
            gathers(ag_first, q)

        def grad(qs, base, js):
            @pl.when(t < last)
            def _():
                gradient([(q, base, j) for q in qs for j in js])

        def drain(q, wide):
            cp = ag_copies(q, wide)
            for copies in [cp['n1'], cp['x']] + cp['n2']:
                send_wait(copies)

        def drained(q):
            send_wait(direct_copies(q))
            gathers(drain, q)

        def put(q):
            def piece(i, carry):
                cc, j = i // (side * side), lax.rem(i, side * side)
                a, b = j // side, lax.rem(j, side)
                d = ((b * side + a) if q % 2 == 0 else (a * side + b)) * CORES + cc
                pltpu.make_async_copy(c_buf.at[q, :, lanes(i * w2, w2)],
                                      r_hbm.at[:, lanes((d * q_all + q) * w2, w2)], out_sem).start()
                return carry

            @pl.when(t == last)
            def _():
                lax.fori_loop(0, CORES * side * side, piece, 0)

        def each(f):
            return lambda qs: [f(q) for q in qs]

        acts = {
            'A': each(lambda q: product(q, True, (0,))), 'B': each(lambda q: product(q, False, (0,))),
            'P': each(lambda q: product(q, True, (1, 2))), 'O': each(lambda q: product(q, False, (1, 2))),
            'p': each(lambda q: product(q, True, (3,))), 'o': each(lambda q: product(q, False, (3,))),
            'S': each(lambda q: pair_sum(q, (0,), 'far')), 'N': each(lambda q: pair_sum(q, (1, 2), 'plain')),
            's': each(lambda q: pair_sum(q, (3,), None)),
            'a': each(ring_mid), 'T': each(ring_sum), 'F': each(finish),
            'c': each(lambda q: gathers(ag_second, q)), 'e': each(lambda q: gathers(ag_third, q)),
            'm': each(lambda q: gathers(ag_mate, q)), 'n': each(lambda q: gathers(ag_mate2, q)),
            'Q': lambda qs: grad(qs, hbase, (3,)), 'G': lambda qs: grad(qs, hbase, (0, 1, 2)),
            'H': lambda qs: grad(qs, pbase, (3,)), 'h': lambda qs: grad(qs, pbase, (0, 1, 2)),
            'D': each(drained), 'R': each(put),
        }
        for act in ' '.join(SCHEDULE).split():
            with jax.named_scope(act):
                acts[act[0]]([int(v) for v in act[1:]])

        @pl.when(t < last)
        def _():
            update = eta_ref[...] * (gacc[...] * (1.0 / n) - (RIDGE_COEF / n) * w_ref[...])
            w_ref[...] = w_ref[...] + MIX_WEIGHT * update
            dwt[...] = update.astype(jnp.bfloat16)
            gacc[...] = jnp.zeros_like(gacc)
        return carry

    lax.fori_loop(0, last + 1, sweep, 0)

    for q in range(q_all):
        pltpu.make_async_copy(c_buf.at[q], c_buf.at[q], out_sem).wait()


def _store(w_in, r_in, w_out, r_out, w_buf, r_buf, w_sem, r_sem):
    width = r_in.shape[1] // PARTS

    def w_copies():
        return pltpu.make_async_copy(w_in, w_buf, w_sem.at[0]), pltpu.make_async_copy(w_buf, w_out, w_sem.at[1])

    def r_copies(i):
        at = pl.ds(i * width, width)
        return (pltpu.make_async_copy(r_in.at[:, at], r_buf.at[i], r_sem.at[0, i]),
                pltpu.make_async_copy(r_buf.at[i], r_out.at[:, at], r_sem.at[1, i]))

    pairs = [w_copies()] + [r_copies(i) for i in range(PARTS)]
    for a, _ in pairs:
        a.start()
    for a, b in pairs:
        a.wait()
        b.start()
    for _, b in pairs:
        b.wait()


def solution(mesh):
    group = mesh.shape['feat']
    side = math.isqrt(group // CORES)

    def local_solve(design, targets, weights, step_sizes):
        n, feats = design.shape
        k = targets.shape[1]
        rows = n // CHUNKS
        half = rows // CORES
        w1 = half // side
        w2 = w1 // side
        f32, bf16 = jnp.float32, jnp.bfloat16
        vm = pl.BlockSpec(memory_space=pltpu.VMEM)
        hb = pl.BlockSpec(memory_space=pl.ANY)
        w_out, r_out = pl.pallas_call(
            functools.partial(_kernel, n, side),
            out_shape=(jax.ShapeDtypeStruct((k, feats), f32), jax.ShapeDtypeStruct((k, n), f32)),
            in_specs=[hb, hb, vm, vm],
            out_specs=(vm, hb),
            scratch_shapes=[
                pltpu.VMEM((CHUNKS, rows, feats), bf16),
                pltpu.VMEM((CHUNKS, k, rows), f32),
                pltpu.VMEM((CHUNKS, k, half), f32),
                pltpu.VMEM((CHUNKS, 2, k, w1 // 2), f32),
                pltpu.VMEM((CHUNKS, 2, k, w1), f32),
                pltpu.VMEM((CHUNKS, 3, k, w2), f32),
                pltpu.VMEM((CHUNKS, k, w1), f32),
                pltpu.VMEM((CHUNKS, k, rows), bf16),
                pltpu.VMEM((CHUNKS, k, w2), f32),
                pltpu.VMEM((k, feats), f32),
                pltpu.VMEM((k, feats), bf16),
                pltpu.VMEM((k, CHUNKS * w2), f32),
                pltpu.SemaphoreType.DMA((CHUNKS, 32)),
                pltpu.SemaphoreType.DMA((CHUNKS, 32)),
                pltpu.SemaphoreType.DMA((CHUNKS, CORES, 4)),
                pltpu.SemaphoreType.DMA,
                pltpu.SemaphoreType.REGULAR((CHUNKS,)),
            ],
            compiler_params=pltpu.CompilerParams(
                collective_id=0, has_side_effects=True, vmem_limit_bytes=67043328),
        )(design, targets.T, weights.T, step_sizes[None, :])
        w_out, r_out = pl.pallas_call(
            _store,
            out_shape=(jax.ShapeDtypeStruct((k, feats), f32), jax.ShapeDtypeStruct((k, n), f32)),
            in_specs=[hb, hb],
            out_specs=(hb, hb),
            scratch_shapes=[
                pltpu.VMEM((k, feats), f32),
                pltpu.VMEM((PARTS, k, n // PARTS), f32),
                pltpu.SemaphoreType.DMA((2,)),
                pltpu.SemaphoreType.DMA((2, PARTS)),
            ],
        )(w_out, r_out)
        return w_out.T, r_out.T

    return jax.shard_map(
        local_solve,
        mesh=mesh,
        in_specs=(P('prob', 'feat'), P('prob', None), P(('prob', 'feat'), None), P(('prob', 'feat'))),
        out_specs=(P(('prob', 'feat'), None), P('prob', None)),
        check_vma=False,
    )
```
